32 devices in a mesh: win: 8 (over z, x), fsdp: 4 (over y, core).
Axes of the slice: x: 2, y: 2, z: 4, core: 2. Of those that a mesh axis runs over, the one named last changes fastest.
Arguments:
- queries: bfloat16 [8192, 2560], P(('win', 'fsdp')), may hold values from -5 to 5
- keys: bfloat16 [8192, 2560], P(('win', 'fsdp')), may hold values from -5 to 5
- values: bfloat16 [8192, 2560], P(('win', 'fsdp')), may hold values from -6 to 6
- stream: bfloat16 [8192, 5120], P(('win', 'fsdp')), may hold values from -0.59765625 to 0.59765625
- out_weight: bfloat16 [2560, 5120], P('fsdp', 'win'), may hold values from -0.125 to 0.125
- gate: float32 [5120], replicated, may hold values from 0.5 to 2
- head_shift: float32 [5120], replicated, may hold values from -3 to 3
- head_scale: float32 [5120], replicated, may hold values from 0.25 to 1.75
- head_weight: bfloat16 [5120, 64], replicated, may hold values from -0.078125 to 0.078125
- latents: float32 [128, 4096], P('win', 'fsdp'), may hold values from -6 to 6
- step_size: float32 [1], replicated, may hold values from 0.5 to 1
- intersections: int32 [8], replicated, may hold values from 1 to 4
- ramps: int32 [8, 4, 2], replicated, may hold values from 1 to 16
Outputs:
- blended: float32 [128, 4096], P('win', 'fsdp')
The draws below stay inside these ranges and needn't reach their ends.
All inputs are finite; a program needn't handle non-finite values.
Results may differ from the reference program's by a relative error of at most 0.0065.
Values may be sent and summed in bfloat16 or wider, within the bound.
No kernel may reach another device: no remote copies, remote signals or barrier semaphores. Data moves between devices by JAX's collectives and lax.ppermute only.
A program may use at most 128 MiB of HBM per device.

```python
import math
import jax
import jax.numpy as jnp
from jax import lax

D = 5120
HEADS = 20
HD = 128
C = 64
P_SIZE = 64
FD = 4
FW = 16
TOKENS = 8192
FRAMES = 128
N_WIN = 8
N_FSDP = 4


def attention_pair(key):
    base = jax.random.fold_in(key, 7)
    first_key, second_key = jax.random.split(base, 2)
    total_rows = N_WIN * FD * N_FSDP * P_SIZE
    columns = HEADS * HD
    query_set = jnp.clip(jax.random.normal(first_key, (total_rows, columns), jnp.float32), -5.0, 5.0)
    key_set = jnp.clip(jax.random.normal(second_key, (total_rows, columns), jnp.float32), -5.0, 5.0)
    return (query_set.astype(jnp.bfloat16), key_set.astype(jnp.bfloat16))


def draw_queries(key, part):
    return attention_pair(key)[0]


def draw_keys(key, part):
    return attention_pair(key)[1]


def set_ends(entries, own_key, least, high):
    dims = entries.shape
    spot = [jax.random.randint(jax.random.fold_in(own_key, axis), (), 0, dims[axis]) for axis in range(len(dims))]
    entries = entries.at[tuple(spot)].set(least)
    longest = dims.index(max(dims))
    spot[longest] = (spot[longest] + 1) % dims[longest]
    return entries.at[tuple(spot)].set(high)


def level_of(stream_key, extent, cuts, least, top_value):
    def one(dim, shards_of):
        steps = jax.random.uniform(jax.random.fold_in(jax.random.fold_in(stream_key, 6), dim), (shards_of,), jnp.float32, least / len(cuts), top_value / len(cuts))
        return jnp.repeat(jnp.exp(steps), extent[dim] // shards_of).reshape((-1,) + (1,) * (len(extent) - dim - 1))

    factor_of = one(*cuts[0])
    for cut in cuts[1:]:
        factor_of = factor_of * one(*cut)
    return factor_of


def noise(own_key, dims, scale, reach, cuts=(), held_as=jnp.bfloat16):
    result = jax.random.normal(own_key, dims, jnp.float32) * scale
    if len(cuts) > 0:
        result = level_of(own_key, dims, cuts, -0.22, 0.18) * result
    return jnp.clip(result, min=-reach, max=reach).astype(held_as)


def setup_inputs(seed: int = 0) -> dict:
    key_list = jax.random.split(jax.random.key(seed), 14)
    queries = draw_queries(jax.random.fold_in(key_list[13], 71), 0)
    keys = draw_keys(jax.random.fold_in(key_list[13], 71), 0)
    values = noise(key_list[2], (TOKENS, HEADS * HD), 1.0, 6.0, ((0, 32),))
    stream = noise(key_list[3], (TOKENS, D), 0.1, 0.59765625, ((0, 32),))
    out_weight = noise(key_list[4], (HEADS * HD, D), (HEADS * HD) ** -0.5, 0.125, ((0, 4), (1, 8)))
    gate = jnp.clip(jax.random.uniform(key_list[5], (D,), jnp.float32, 0.5, 2.0), 0.5, 2.0)
    head_shift = noise(key_list[6], (D,), 0.5, 3.0, (), jnp.float32)
    head_scale = jnp.clip(1.0 + 0.15 * jax.random.normal(key_list[7], (D,), jnp.float32), 0.25, 1.75)
    head_weight = noise(key_list[8], (D, C), D ** -0.5, 0.078125)
    latents = noise(key_list[9], (FRAMES, P_SIZE * C), 1.0, 6.0, ((0, 8), (1, 4)), jnp.float32)
    step_size = jnp.clip(jax.random.uniform(key_list[10], (1,), jnp.float32, 0.5, 1.0), 0.5, 1.0)
    intersections = set_ends(jax.random.randint(key_list[11], (N_WIN,), 1, FD + 1), jax.random.fold_in(key_list[11], 1), 1, FD).astype(jnp.int32)
    ramps = set_ends(jax.random.randint(key_list[12], (N_WIN, FD, 2), 1, 17), jax.random.fold_in(key_list[12], 1), 1, 16).astype(jnp.int32)
    return {"queries": queries, "keys": keys, "values": values, "stream": stream, "out_weight": out_weight, "gate": gate, "head_shift": head_shift, "head_scale": head_scale, "head_weight": head_weight, "latents": latents, "step_size": step_size, "intersections": intersections, "ramps": ramps}


EPSILON = 0.001

def attend(window_parts):
    query_win, key_win, value_win = window_parts
    window_tokens = FW * P_SIZE
    query_h = query_win.reshape(window_tokens, HEADS, HD).astype(jnp.float32)
    key_h = key_win.reshape(window_tokens, HEADS, HD).astype(jnp.float32)
    value_h = value_win.reshape(window_tokens, HEADS, HD).astype(jnp.float32)
    scores = jnp.einsum('qhd,khd->hqk', query_h, key_h) * (1.0 / math.sqrt(HD))
    highest = lax.optimization_barrier(jnp.max(scores, axis=-1, keepdims=True))
    exponent = jnp.exp(scores - highest)
    denominator = lax.optimization_barrier(jnp.sum(exponent, axis=-1))
    probability = exponent.astype(jnp.bfloat16)
    probability = lax.optimization_barrier(probability).astype(jnp.float32)
    summed = jnp.einsum('hqk,khd->qhd', probability, value_h)
    attended = summed / jnp.transpose(denominator)[:, :, None]
    return attended.reshape(window_tokens, HEADS * HD).astype(jnp.bfloat16)

def reference(queries, keys, values, stream, out_weight, gate, head_shift, head_scale, head_weight, latents, step_size, intersections, ramps):
    window_tokens = FW * P_SIZE
    feat_width = HEADS * HD
    attended = lax.map(attend, (queries.reshape(N_WIN, window_tokens, feat_width), keys.reshape(N_WIN, window_tokens, feat_width), values.reshape(N_WIN, window_tokens, feat_width)))
    attended = attended.reshape(N_WIN * window_tokens, feat_width)
    projected = jnp.dot(attended, out_weight, preferred_element_type=jnp.float32)
    hidden = stream.astype(jnp.float32) + gate * projected
    centre = lax.optimization_barrier(jnp.mean(hidden, axis=-1, keepdims=True))
    centred = hidden - centre
    variance = lax.optimization_barrier(jnp.mean(centred * centred, axis=-1, keepdims=True))
    normed = centred / jnp.sqrt(variance + EPSILON)
    modulated = (normed * head_scale + head_shift).astype(jnp.bfloat16)
    velocity = jnp.dot(modulated, head_weight, preferred_element_type=jnp.float32)
    velocity = velocity.reshape(N_WIN, N_FSDP, FW, P_SIZE // N_FSDP, C)
    velocity = jnp.transpose(velocity, (0, 2, 1, 3, 4)).reshape(N_WIN * FW, P_SIZE * C)
    fresh = latents + step_size[0] * velocity
    frames_all = fresh.reshape(N_WIN, FW, P_SIZE * C)
    frame_ids = jnp.arange(FW, dtype=jnp.int32)
    over_prev = jnp.roll(intersections, 1).astype(jnp.int32)
    over_next = intersections.astype(jnp.int32)
    ramp_prev = jnp.roll(ramps, 1, axis=0).astype(jnp.float32)
    ramp_own = ramps.astype(jnp.float32)
    before_win = jnp.roll(frames_all, 1, axis=0)
    after_win = jnp.roll(frames_all, -1, axis=0)
    source_prev = jnp.clip(FW - over_prev[:, None] + frame_ids[None, :], 0, FW - 1).astype(jnp.int32)
    prev_aligned = jnp.take_along_axis(before_win, source_prev[:, :, None], axis=1)
    inside_prev = frame_ids[None, :] < over_prev[:, None]
    prev_index = jnp.minimum(frame_ids, FD - 1).astype(jnp.int32)
    weight_before = ramp_prev[:, prev_index, 0]
    weight_self = ramp_prev[:, prev_index, 1]
    blend_prev = (weight_before[:, :, None] * prev_aligned + weight_self[:, :, None] * frames_all) / (weight_before + weight_self)[:, :, None]
    shifted = frame_ids[None, :] - (FW - over_next[:, None])
    inside_next = shifted >= 0
    source_next = jnp.clip(shifted, 0, FW - 1).astype(jnp.int32)
    next_aligned = jnp.take_along_axis(after_win, source_next[:, :, None], axis=1)
    next_index = jnp.clip(shifted, 0, FD - 1).astype(jnp.int32)
    weight_mine = jnp.take_along_axis(ramp_own[:, :, 0], next_index, axis=1)
    weight_after = jnp.take_along_axis(ramp_own[:, :, 1], next_index, axis=1)
    blend_next = (weight_mine[:, :, None] * frames_all + weight_after[:, :, None] * next_aligned) / (weight_mine + weight_after)[:, :, None]
    blended = jnp.where(inside_prev[:, :, None], blend_prev, jnp.where(inside_next[:, :, None], blend_next, frames_all))
    return blended.reshape(N_WIN * FW, P_SIZE * C)
```

```python
import functools
import math

import jax
import jax.numpy as jnp
from jax import lax
from jax.experimental import pallas as pl
from jax.experimental.pallas import tpu as pltpu
from jax.sharding import PartitionSpec as P


HD = 128
FD = 4
EPSILON = 0.001
LANES = 128


def swap(value, axis, bits):
    size = lax.axis_size(axis)
    return lax.ppermute(value, axis, [(i, i ^ bits) for i in range(size)])


def line_move(value, moves):
    pairs = [(2 * a + p, 2 * b + p) for a, b in moves for p in range(2)]
    return lax.ppermute(value, "win", pairs)


def attend_kernel(score_scale, ids, q_ref, k_ref, v_ref, mate_ref, far_ref, diag_ref, out_ref):
    keys = [k_ref[...], mate_ref[0, 1], far_ref[0], diag_ref[0]]
    values = [v_ref[...], mate_ref[0, 2], far_ref[1], diag_ref[1]]
    factor = score_scale * math.log2(math.e)
    for half, query in enumerate((q_ref[...], mate_ref[0, 0])):
        scores = [
            lax.dot_general(query, k, (((1,), (1,)), ((), ())), preferred_element_type=jnp.float32)
            for k in keys
        ]
        peaks = [jnp.max(s, axis=-1, keepdims=True) for s in scores]
        highest = functools.reduce(jnp.maximum, peaks)
        total = None
        summed = None
        for s, v in zip(scores, values):
            exponent = jnp.exp2((s - highest) * factor)
            part = jnp.sum(exponent, axis=-1, keepdims=True)
            prod = jnp.dot(exponent.astype(jnp.bfloat16), v, preferred_element_type=jnp.float32)
            total = part if total is None else total + part
            summed = prod if summed is None else summed + prod
        out_ref[half] = (summed / total).astype(jnp.bfloat16)


def attend(ids, queries, keys, values, mate, far, diag, part, first, count, heads):
    rows = queries.shape[0]
    wide = pl.BlockSpec((rows, HD), lambda h, ids: (0, ids[part] * heads + first + h))
    narrow = pl.BlockSpec((2, rows, HD), lambda h, ids: (0, 0, h))
    return pl.pallas_call(
        functools.partial(attend_kernel, 1.0 / math.sqrt(HD)),
        grid_spec=pltpu.PrefetchScalarGridSpec(
            num_scalar_prefetch=1,
            grid=(count,),
            in_specs=[wide] * 3
            + [pl.BlockSpec((1, 3, rows, HD), lambda h, ids: (part, 0, 0, first + h))]
            + [narrow] * 2,
            out_specs=narrow,
        ),
        out_shape=jax.ShapeDtypeStruct((2, rows, count * HD), jnp.bfloat16),
        cost_estimate=pl.CostEstimate(
            flops=32 * rows * rows * HD * count,
            bytes_accessed=24 * rows * HD * count,
            transcendentals=8 * rows * rows * count,
        ),
    )(ids, queries, keys, values, mate, far, diag)


def fetch_weights(picks, ids, sources, held, sems):
    copies = []
    at = 0
    for j, pick in enumerate(picks):
        for c in range(pick):
            copy = pltpu.make_async_copy(sources[at + c], held.at[j], sems.at[j])
            if pick == 1:
                pl.when(pl.program_id(0) == 0)(copy.start)
            else:
                pl.when((pl.program_id(0) == 0) & (ids[j] == c))(copy.start)
        copies.append(pltpu.make_async_copy(sources[at], held.at[j], sems.at[j]))
        at += pick
    return copies


def projected(att, held, slot, depth):
    total = None
    start = 0
    for part in att:
        cols = part.shape[-1]
        weight = held[2 * slot + start // depth, pl.ds(start % depth, cols), :]
        term = jnp.dot(part[0], weight, preferred_element_type=jnp.float32)
        total = term if total is None else total + term
        start += cols
    return total


def give_kernel(picks, chunks, ids, *refs):
    att = refs[: 2 * chunks]
    sources = refs[2 * chunks : 2 * chunks + sum(picks)]
    give_ref, held, sems = refs[2 * chunks + sum(picks) :]
    depth = held.shape[1]
    copies = fetch_weights(picks, ids, sources, held, sems)
    for b in range(len(picks) // 2):
        @pl.when(pl.program_id(0) == b)
        def _():
            copies[2 * b].wait()
            copies[2 * b + 1].wait()
            for w in range(2):
                part = projected(att[w * chunks : (w + 1) * chunks], held, b, depth)
                give_ref[0, w] = part.astype(jnp.bfloat16)


def weight_specs(att, half, sources):
    spec = lambda v: pl.BlockSpec((1,) + v.shape[1:], lambda b, ids: (half, 0, 0))
    return [spec(v) for v in att] + [pl.BlockSpec(memory_space=pl.ANY)] * sum(
        len(s) for s in sources
    )


def give(ids, att, sources):
    rows = att[0].shape[1]
    depth, span = sources[0][0].shape
    slots = len(sources)
    return pl.pallas_call(
        functools.partial(give_kernel, tuple(len(s) for s in sources), len(att) // 2),
        grid_spec=pltpu.PrefetchScalarGridSpec(
            num_scalar_prefetch=1,
            grid=(slots // 2,),
            in_specs=weight_specs(att, 1, sources),
            out_specs=pl.BlockSpec((1, 2, rows, span), lambda b, ids: (b, 0, 0, 0)),
            scratch_shapes=[
                pltpu.VMEM((slots, depth, span), jnp.bfloat16),
                pltpu.SemaphoreType.DMA((slots,)),
            ],
        ),
        out_shape=jax.ShapeDtypeStruct((slots // 2, 2, rows, span), jnp.bfloat16),
        cost_estimate=pl.CostEstimate(
            flops=4 * rows * depth * span * slots,
            bytes_accessed=8 * rows * depth + 2 * slots * depth * span,
            transcendentals=0,
        ),
    )(ids, *att, *(o for s in sources for o in s))


def tally_kernel(picks, chunks, first, ids, *refs):
    att = refs[: 2 * chunks]
    sources = refs[2 * chunks : 2 * chunks + sum(picks)]
    got_ref, own_ref, other_ref, gate_ref, scale_ref, head_ref, old_ref, out_ref, held, sems = refs[
        2 * chunks + sum(picks) :
    ]
    depth = held.shape[1]
    rows = own_ref.shape[0]
    head = head_ref[0]
    chans = head.shape[1]
    copies = fetch_weights(picks, ids, sources, held, sems)
    for b in range(len(picks) // 2):
        @pl.when(pl.program_id(0) == b)
        def _():
            copies[2 * b].wait()
            copies[2 * b + 1].wait()
            for w, stream in enumerate((own_ref[...], other_ref[0])):
                proj = projected(att[w * chunks : (w + 1) * chunks], held, b, depth)
                proj = proj + got_ref[0, w].astype(jnp.float32)
                hidden = stream.astype(jnp.float32) + gate_ref[0] * proj
                at = pl.ds(w * rows, rows)
                fresh = first and b == 0
                if fresh:
                    centre = jnp.mean(hidden, axis=-1, keepdims=True)
                else:
                    old = (old_ref if b == 0 else out_ref)[at, :]
                    centre = old[:, chans : chans + 1]
                moved = hidden - centre
                dots = jnp.dot(
                    (moved * scale_ref[0]).astype(jnp.bfloat16),
                    head,
                    preferred_element_type=jnp.float32,
                )
                one = jnp.sum(moved, axis=-1, keepdims=True)
                two = jnp.sum(moved * moved, axis=-1, keepdims=True)
                if not fresh:
                    dots = dots + old[:, :chans]
                    one = one + old[:, chans + 1 : chans + 2]
                    two = two + old[:, chans + 2 : chans + 3]
                out_ref[at, :chans] = dots
                lane = lax.broadcasted_iota(jnp.int32, (rows, out_ref.shape[1] - chans), 1)
                out_ref[at, chans:] = jnp.where(
                    lane == 0, centre, jnp.where(lane == 1, one, jnp.where(lane == 2, two, 0.0))
                )


def tally(ids, att, sources, got, own, other, gate, scale, head, stats):
    rows = att[0].shape[1]
    depth, span = sources[0][0].shape
    chans = head.shape[2]
    slots = len(sources)
    by_block = lambda shape: pl.BlockSpec((1,) + shape, lambda b, ids: (ids[slots + b], 0, 0))
    lanes = chans + LANES - chans % LANES
    first = stats is None
    if first:
        stats = jnp.zeros((8, LANES), jnp.float32)
    return pl.pallas_call(
        functools.partial(tally_kernel, tuple(len(s) for s in sources), len(att) // 2, first),
        grid_spec=pltpu.PrefetchScalarGridSpec(
            num_scalar_prefetch=1,
            grid=(slots // 2,),
            in_specs=weight_specs(att, 0, sources)
            + [
                pl.BlockSpec((1, 2, rows, span), lambda b, ids: (b, 0, 0, 0)),
                pl.BlockSpec((rows, span), lambda b, ids: (0, ids[slots + b])),
                pl.BlockSpec((1, rows, span), lambda b, ids: (ids[slots + slots // 2 + b], 0, 0)),
            ]
            + [by_block((1, span))] * 2
            + [
                by_block((span, chans)),
                pl.BlockSpec(stats.shape, lambda b, ids: (0, 0)),
            ],
            out_specs=pl.BlockSpec((2 * rows, lanes), lambda b, ids: (0, 0)),
            scratch_shapes=[
                pltpu.VMEM((slots, depth, span), jnp.bfloat16),
                pltpu.SemaphoreType.DMA((slots,)),
            ],
        ),
        out_shape=jax.ShapeDtypeStruct((2 * rows, lanes), jnp.float32),
        cost_estimate=pl.CostEstimate(
            flops=4 * rows * depth * span * slots,
            bytes_accessed=8 * rows * depth + 2 * slots * depth * span,
            transcendentals=0,
        ),
    )(ids, *att, *(o for s in sources for o in s), got, own, other, gate, scale, head, stats)


def after(value, *marks):
    return lax.optimization_barrier((value,) + marks)[0]


def blend_weights(intersections, ramps, frames):
    window = lax.axis_index("win")
    count = lax.axis_size("win")
    prev_window = (window + count - 1) % count
    over_prev = lax.dynamic_index_in_dim(intersections, prev_window, keepdims=False)
    over_next = lax.dynamic_index_in_dim(intersections, window, keepdims=False)
    ramp_prev = lax.dynamic_index_in_dim(ramps, prev_window, keepdims=False).astype(jnp.float32)
    ramp_own = lax.dynamic_index_in_dim(ramps, window, keepdims=False).astype(jnp.float32)
    frame = jnp.arange(frames, dtype=jnp.int32)[:, None]
    shared = jnp.arange(FD, dtype=jnp.int32)[None, :]
    share_prev = ramp_prev / (ramp_prev[:, 0:1] + ramp_prev[:, 1:2])
    share_own = ramp_own / (ramp_own[:, 0:1] + ramp_own[:, 1:2])
    inside_prev = frame < over_prev
    at_prev = inside_prev & (shared == frame)
    take_prev = inside_prev & (shared == FD - over_prev + frame)
    weight_before = jnp.sum(jnp.where(at_prev, share_prev[None, :, 0], 0.0), axis=1, keepdims=True)
    self_prev = jnp.sum(jnp.where(at_prev, share_prev[None, :, 1], 0.0), axis=1, keepdims=True)
    place = frame - (frames - over_next)
    inside_next = (place >= 0) & ~inside_prev
    at_next = inside_next & (shared == place)
    self_next = jnp.sum(jnp.where(at_next, share_own[None, :, 0], 0.0), axis=1, keepdims=True)
    coef_prev = jnp.where(take_prev, weight_before, 0.0)
    coef_next = jnp.where(at_next, share_own[None, :, 1], 0.0)
    own = jnp.where(inside_prev, self_prev, jnp.where(inside_next, self_next, 1.0))
    return own, coef_prev, coef_next


def local(
    queries,
    keys,
    values,
    stream,
    out_weight,
    gate,
    head_shift,
    head_scale,
    head_weight,
    latents,
    step_size,
    intersections,
    ramps,
):
    rows, feat = queries.shape
    groups = lax.axis_size("fsdp")
    count = lax.axis_size("win")
    line = count // 2
    width = out_weight.shape[1]
    model = stream.shape[1]
    chans = head_weight.shape[1]
    cols = feat // groups
    heads = cols // HD
    window = lax.axis_index("win")
    member = lax.axis_index("fsdp")
    z = window // 2
    parity = window % 2
    regroup = width % LANES != 0 or line != 4
    blocks = line
    if regroup:
        blocks = max(b for b in (1, 2, 4) if (model // 2) % (b * LANES) == 0)
    span = model // 2 // blocks

    def group(value, bits):
        return lax.dynamic_slice(value, (0, (member ^ bits) * cols), (rows, cols))

    def pack(bits, *arrays):
        return jnp.stack([group(v, bits) for v in arrays])

    ids = jnp.stack([member, member ^ 2]).astype(jnp.int32)
    if regroup:
        sets = [[2 * a + p for a in range(line)] for p in range(2)]
        full = lax.all_gather(out_weight, "win", axis=1, tiled=True, axis_index_groups=sets)
        near = [[full[:, r * span : (r + 1) * span]] for r in range(blocks)]
        far = [[swap(b[0], "fsdp", 2)] for b in near]
        picks = [0] * blocks
        half_first = lambda v: jnp.swapaxes(v.reshape((line, 2, width) + v.shape[1:]), 0, 1)
        places = [(parity * blocks + r, r) for r in range(blocks)]
        ordered = half_first(stream.T).reshape(model, rows).T
        sent = [(1 - parity) * blocks + r for r in range(blocks)]
    else:
        down = [(a + 1, a) for a in range(line - 1)]
        up = [(a, a + 1) for a in range(line - 1)]
        on_down = [(a - 1, a - 2) for a in range(2, line)]
        on_up = [(a + 1, a + 2) for a in range(line - 2)]
        far_w = swap(out_weight, "fsdp", 2)
        near_up = line_move(out_weight, up)
        near_down = line_move(out_weight, down)
        half_first = lambda v: v
        ordered = stream
        sent = [2 * r + 1 - parity for r in range(blocks)]
    sizes = [(0, 0, heads), (1, 0, (heads + 1) // 2), (1, (heads + 1) // 2, heads // 2)]

    def sends(chunk, mark):
        part, first, size = chunk
        at = slice(first * HD, (first + size) * HD)
        direct = pack(2 if part == 0 else 0, keys, values)[:, :, at]
        cross = pack(3 if part == 0 else 1, keys, values)[:, :, at]
        if mark is not None:
            direct, cross = after((direct, cross), mark)
        return swap(direct, "fsdp", 2), swap(cross, "fsdp", 3)

    kv0 = sends(sizes[0], None)
    mate = swap(
        jnp.stack([pack(1, queries, keys, values), pack(3, queries, keys, values)]), "fsdp", 1
    )
    other_stream = swap(
        jnp.stack([lax.dynamic_slice(ordered, (0, b * span), (rows, span)) for b in sent]), "win", 1
    )
    if not regroup:
        up2 = line_move(near_up, on_up)
        down2 = line_move(near_down, on_down)
        near2 = jnp.where(z >= 2, up2, down2)
        edge = line_move(near2, [(2, 3), (1, 0)])
        far_up = line_move(far_w, up)
        far_down = line_move(far_w, down)
    kv1 = sends(sizes[1], kv0)

    def run(chunk, kv):
        return attend(ids, queries, keys, values, mate, *kv, *chunk, heads)

    att0 = run(sizes[0], kv0)
    att0_x = swap(att0, "win", 1)
    kv2 = sends(sizes[2], kv1)
    att1 = run(sizes[1], kv1)
    att1_x = swap(att1, "win", 1)
    if not regroup:
        ends = [
            ((w * groups + f), (w * groups + (f ^ 2)))
            for w in range(count)
            if w // 2 in (0, line - 1)
            for f in range(groups)
        ]
        edge, far_up, far_down = after((edge, far_up, far_down), att1)
        far_edge = lax.ppermute(edge, ("win", "fsdp"), ends)
        far_up2 = line_move(far_up, on_up)
        far_down2 = line_move(far_down, on_down)
        at_top = (z == line - 1).astype(jnp.int32)
        at_end = ((z == line - 1) | (z == 0)).astype(jnp.int32)
        upper = (z >= 2).astype(jnp.int32)
        near = [[out_weight], [near_down, near_up], [near2], [near_up, edge]]
        far = [[far_w], [far_down, far_up], [far_down2, far_up2], [far_up, far_edge]]
        picks = [(0, 0), (at_top, at_top), (0, upper), (at_end, at_end)]
        steps = [0, jnp.where(z == line - 1, 3, 1), 2, jnp.where(z == line - 1, 1, 3)]
        places = [(2 * ((z + r) % line) + parity, (z + r) % line) for r in steps]
    else:
        picks = [(0, 0)] * blocks
    att2 = run(sizes[2], kv2)
    att2_x = swap(att2, "win", 1)
    att = (att0, att1, att2, att0_x, att1_x, att2_x)

    gate_b = half_first(gate).reshape(2 * blocks, 1, span)
    scale_b = half_first(head_scale).reshape(2 * blocks, 1, span)
    head_b = half_first(head_weight).reshape(2 * blocks, span, chans)
    each = 2 if blocks % 2 == 0 else 1
    calls = []
    for first in range(0, blocks, each):
        now = range(first, first + each)
        sources = [s[b] for b in now for s in (near, far)]
        chosen = [p for b in now for p in picks[b]]
        chosen += [places[b][i] for i in range(2) for b in now]
        chosen = jnp.stack([jnp.asarray(c, jnp.int32) for c in chosen])
        sent = give(chosen, att, sources)
        calls.append((chosen, sources, swap(sent, "fsdp", 1)))
    stats = None
    for chosen, sources, got in calls:
        stats = tally(
            chosen, att, sources, got, ordered, other_stream, gate_b, scale_b, head_b, stats
        )

    mine = stats[:rows]
    theirs = swap(stats[rows:], "win", 1)
    head_f = head_weight.astype(jnp.float32)
    scaled = (head_scale[:, None] * head_f).reshape(line, 2, width, chans)
    per_half = jnp.sum(scaled, axis=(0, 2))
    own_cw = lax.dynamic_index_in_dim(per_half, parity, keepdims=True)
    their_cw = lax.dynamic_index_in_dim(per_half, 1 - parity, keepdims=True)
    offset = jnp.sum(head_shift[:, None] * head_f, axis=0, keepdims=True)
    half = model // 2

    def fields(s):
        return s[:, :chans], s[:, chans : chans + 1], s[:, chans + 1 : chans + 2], s[:, chans + 2 : chans + 3]

    dot_a, mid_a, one_a, two_a = fields(mine)
    dot_b, mid_b, one_b, two_b = fields(theirs)
    centre = (one_a + one_b) / model + 0.5 * (mid_a + mid_b)
    da = centre - mid_a
    db = centre - mid_b
    square = (two_a - 2.0 * da * one_a + half * da * da) + (two_b - 2.0 * db * one_b + half * db * db)
    inverse = 1.0 / jnp.sqrt(square / model + EPSILON)
    velocity = (dot_a + dot_b - da * own_cw - db * their_cw) * inverse + offset
    fresh = latents + step_size[0] * velocity.reshape(latents.shape)
    frames = latents.shape[0]

    up = [(i, (i + 1) % count) for i in range(count)]
    down = [(j, i) for i, j in up]
    sent = fresh.astype(jnp.bfloat16)
    tail = lax.ppermute(sent[frames - FD :], "win", up).astype(jnp.float32)
    start = lax.ppermute(sent[:FD], "win", down).astype(jnp.float32)
    own, coef_prev, coef_next = blend_weights(intersections, ramps, frames)
    out = own * fresh
    for j in range(FD):
        out = out + coef_prev[:, j : j + 1] * tail[j : j + 1]
        out = out + coef_next[:, j : j + 1] * start[j : j + 1]
    return out


def solution(mesh):
    in_specs = (
        P(("win", "fsdp"), None),
        P(("win", "fsdp"), None),
        P(("win", "fsdp"), None),
        P(("win", "fsdp"), None),
        P("fsdp", "win"),
        P(),
        P(),
        P(),
        P(),
        P("win", "fsdp"),
        P(),
        P(),
        P(),
    )
    out_specs = P("win", "fsdp")

    return jax.shard_map(local, mesh=mesh, in_specs=in_specs, out_specs=out_specs, check_vma=False)
```

```python
import functools
import math

import jax
import jax.numpy as jnp
from jax import lax
from jax.experimental import pallas as pl
from jax.experimental.pallas import tpu as pltpu
from jax.sharding import PartitionSpec as P


HD = 128
FD = 4
EPSILON = 0.001
LANES = 128


WHOLE = pltpu.CompilerParams(vmem_limit_bytes=67043328)


def swap(value, axis, bits):
    size = lax.axis_size(axis)
    return lax.ppermute(value, axis, [(i, i ^ bits) for i in range(size)])


def line_move(value, moves):
    pairs = [(2 * a + p, 2 * b + p) for a, b in moves for p in range(2)]
    return lax.ppermute(value, "win", pairs)


def attend_kernel(score_scale, ids, q_ref, k_ref, v_ref, mate_ref, far_ref, diag_ref, out_ref):
    keys = [k_ref[...], mate_ref[0, 1], far_ref[0], diag_ref[0]]
    values = [v_ref[...], mate_ref[0, 2], far_ref[1], diag_ref[1]]
    factor = score_scale * math.log2(math.e)
    for half, query in enumerate((q_ref[...], mate_ref[0, 0])):
        scores = [
            lax.dot_general(query, k, (((1,), (1,)), ((), ())), preferred_element_type=jnp.float32)
            for k in keys
        ]
        peaks = [jnp.max(s, axis=-1, keepdims=True) for s in scores]
        highest = functools.reduce(jnp.maximum, peaks)
        total = None
        summed = None
        for s, v in zip(scores, values):
            exponent = jnp.exp2((s - highest) * factor)
            part = jnp.sum(exponent, axis=-1, keepdims=True)
            prod = jnp.dot(exponent.astype(jnp.bfloat16), v, preferred_element_type=jnp.float32)
            total = part if total is None else total + part
            summed = prod if summed is None else summed + prod
        out_ref[half] = (summed / total).astype(jnp.bfloat16)


def attend(ids, queries, keys, values, mate, far, diag, part, first, count, heads):
    rows = queries.shape[0]
    wide = pl.BlockSpec((rows, HD), lambda h, ids: (0, ids[part] * heads + first + h))
    narrow = pl.BlockSpec((2, rows, HD), lambda h, ids: (0, 0, h))
    return pl.pallas_call(
        functools.partial(attend_kernel, 1.0 / math.sqrt(HD)),
        grid_spec=pltpu.PrefetchScalarGridSpec(
            num_scalar_prefetch=1,
            grid=(count,),
            in_specs=[wide] * 3
            + [pl.BlockSpec((1, 3, rows, HD), lambda h, ids: (part, 0, 0, first + h))]
            + [narrow] * 2,
            out_specs=narrow,
        ),
        out_shape=jax.ShapeDtypeStruct((2, rows, count * HD), jnp.bfloat16),
        compiler_params=WHOLE,
        cost_estimate=pl.CostEstimate(
            flops=32 * rows * rows * HD * count,
            bytes_accessed=24 * rows * HD * count,
            transcendentals=8 * rows * rows * count,
        ),
    )(ids, queries, keys, values, mate, far, diag)


class Fetch:
    def __init__(self, sems):
        self.sems = sems
        self.count = 0

    def start(self, source, target):
        copy = pltpu.make_async_copy(source, target, self.sems.at[self.count])
        self.count += 1
        copy.start()
        return copy

    def start_one_of(self, index, sources, target):
        copies = [pltpu.make_async_copy(v, target, self.sems.at[self.count]) for v in sources]
        self.count += 1
        for c, copy in enumerate(copies):
            if len(copies) == 1:
                copy.start()
            else:
                pl.when(index == c)(copy.start)
        return copies[0]


def project_kernel(halves, picks, chunks, added, ids, *refs):
    blocks = len(picks)
    att = refs[: 2 * chunks]
    at = 2 * chunks + sum(sum(p) for p in picks)
    sources = list(refs[2 * chunks : at])
    part_ref = refs[at] if added else None
    out_ref, side, held, made, before, sems, out_sems = refs[at + added :]
    rows = side.shape[2]
    depth = held.shape[1] // len(picks[0])
    fetch = Fetch(sems)
    coming = []
    for w in range(2):
        start = 0
        for part in att[w * chunks : (w + 1) * chunks]:
            cols = part.shape[-1]
            source = part if len(halves) == 2 else part.at[pl.ds(halves[0], 1)]
            coming.append(fetch.start(source, side.at[:, w, :, pl.ds(start, cols)]))
            start += cols

    def weights(b):
        waits = []
        for j, pick in enumerate(picks[b]):
            options = [sources.pop(0) for _ in range(pick)]
            place = held.at[b, pl.ds(j * depth, depth), :]
            waits.append(fetch.start_one_of(ids[len(picks[0]) * b + j], options, place))
        if added:
            waits.append(fetch.start(part_ref.at[b, halves[0]], before.at[b]))
        return waits

    queue = [coming + weights(0)] + [weights(b) for b in range(1, min(blocks, 2))]
    leaving = []
    for b in range(blocks):
        for copy in queue[b]:
            copy.wait()
        if b + 2 < blocks:
            queue.append(weights(b + 2))
        for h in range(len(halves)):
            both = side[h].reshape(2 * rows, side.shape[3])
            part = jnp.dot(both, held[b], preferred_element_type=jnp.float32)
            for w in range(2):
                piece = part[w * rows : (w + 1) * rows]
                if added:
                    piece = piece + before[b, w].astype(jnp.float32)
                made[b, h, w] = piece.astype(jnp.bfloat16)
            copy = pltpu.make_async_copy(made.at[b, h], out_ref.at[b, h], out_sems.at[b, h])
            copy.start()
            leaving.append(copy)
    for copy in leaving:
        copy.wait()


def project(ids, halves, att, sources, added=None):
    rows = att[0].shape[1]
    depth, span = sources[0][0][0].shape
    blocks = len(sources)
    picks = tuple(tuple(len(o) for o in block) for block in sources)
    width = depth * len(picks[0])
    flat = [v for block in sources for options in block for v in options]
    shape = (blocks, len(halves), 2, rows, span)
    extra = [] if added is None else [added]
    hbm = pl.BlockSpec(memory_space=pltpu.HBM)
    return pl.pallas_call(
        functools.partial(project_kernel, halves, picks, len(att) // 2, len(extra)),
        in_specs=[pl.BlockSpec(memory_space=pltpu.SMEM)]
        + [hbm] * (len(att) + len(flat) + len(extra)),
        out_specs=hbm,
        scratch_shapes=[
            pltpu.VMEM((len(halves), 2, rows, width), jnp.bfloat16),
            pltpu.VMEM((blocks, width, span), jnp.bfloat16),
            pltpu.VMEM(shape, jnp.bfloat16),
            pltpu.VMEM((blocks if extra else 1, 2, rows, span), jnp.bfloat16),
            pltpu.SemaphoreType.DMA((len(att) + blocks * (len(picks[0]) + 1),)),
            pltpu.SemaphoreType.DMA((blocks, len(halves))),
        ],
        out_shape=jax.ShapeDtypeStruct(shape, jnp.bfloat16),
        compiler_params=WHOLE,
        cost_estimate=pl.CostEstimate(
            flops=4 * rows * len(halves) * width * span * blocks,
            bytes_accessed=8 * rows * width + 2 * blocks * width * span,
            transcendentals=0,
        ),
    )(ids, *att, *flat, *extra)


def tally_kernel(first, last, ids, keep_ref, got_ref, own_ref, other_ref, gate_ref, scale_ref, head_ref, *refs):
    state_ref = None if first else refs[0]
    out_refs = refs[(not first) : -6]
    keep, got, own, other, head, sems = refs[-6:]
    blocks, _, rows, span = keep.shape
    chans = head_ref.shape[2]
    fetch = Fetch(sems)
    place = [ids[b] for b in range(blocks)]
    coming = []
    for b in range(blocks):
        column = pl.ds(pl.multiple_of(place[b] * span, LANES), span)
        coming.append(
            [
                fetch.start(keep_ref.at[b, 0], keep.at[b]),
                fetch.start(got_ref.at[b, 0], got.at[b]),
                fetch.start(own_ref.at[:, column], own.at[b]),
                fetch.start(other_ref.at[ids[blocks + b]], other.at[b]),
                fetch.start(head_ref.at[place[b]], head.at[b]),
            ]
        )
    state = [None] * 2
    if not first:
        for w in range(2):
            old = state_ref[w]
            parts = [old[:, chans + i : chans + i + 1] for i in range(3)]
            state[w] = tuple(parts) + (old[:, :chans],)
    for b in range(blocks):
        for copy in coming[b]:
            copy.wait()
        gate = gate_ref[place[b]]
        scale = scale_ref[place[b]]
        for w, stream in enumerate((own, other)):
            proj = keep[b, w].astype(jnp.float32) + got[b, w].astype(jnp.float32)
            hidden = stream[b].astype(jnp.float32) + gate * proj
            if state[w] is None:
                centre = jnp.mean(hidden, axis=-1, keepdims=True)
            else:
                centre = state[w][0]
            moved = hidden - centre
            dots = jnp.dot(
                (moved * scale).astype(jnp.bfloat16), head[b], preferred_element_type=jnp.float32
            )
            one = jnp.sum(moved, axis=-1, keepdims=True)
            two = jnp.sum(moved * moved, axis=-1, keepdims=True)
            if state[w] is not None:
                one, two, dots = one + state[w][1], two + state[w][2], dots + state[w][3]
            state[w] = (centre, one, two, dots)
    sums_ref = out_refs[0]
    for w, (centre, one, two, dots) in enumerate(state):
        sums_ref[w, :, :chans] = dots
        lane = lax.broadcasted_iota(jnp.int32, (rows, sums_ref.shape[2] - chans), 1)
        sums_ref[w, :, chans:] = jnp.where(
            lane == 0, centre, jnp.where(lane == 1, one, jnp.where(lane == 2, two, 0.0))
        )
    if last:
        across_ref, ahead_ref, behind_ref, beside_ref = out_refs[1:]
        edge = ahead_ref.shape[0]
        odd = ids[2 * blocks]
        inner = pl.ds(pl.multiple_of((1 - odd) * (rows - edge), 8), edge)
        outer = pl.ds(pl.multiple_of(odd * (rows - edge), 8), edge)
        across_ref[:rows] = sums_ref[1]
        across_ref[rows:] = sums_ref[0, inner]
        ahead_ref[...] = sums_ref[1, inner]
        behind_ref[...] = sums_ref[0, outer]
        beside_ref[...] = sums_ref[1, outer]


def tally(ids, keep, got, own, other, gate, scale, head, state, edge):
    blocks, _, _, rows, span = keep.shape
    chans = head.shape[2]
    lanes = chans + LANES - chans % LANES
    old = [] if state is None else [state]
    anywhere = pl.BlockSpec(memory_space=pltpu.HBM)
    near_by = pl.BlockSpec(memory_space=pltpu.VMEM)
    shapes = [(2, rows, lanes)]
    if edge:
        shapes += [(rows + edge, lanes)] + [(edge, lanes)] * 3
    return pl.pallas_call(
        functools.partial(tally_kernel, state is None, edge > 0),
        in_specs=[pl.BlockSpec(memory_space=pltpu.SMEM)]
        + [anywhere] * 4
        + [near_by] * 2
        + [anywhere]
        + [near_by] * len(old),
        out_specs=[near_by] * len(shapes),
        scratch_shapes=[
            pltpu.VMEM((blocks, 2, rows, span), jnp.bfloat16),
            pltpu.VMEM((blocks, 2, rows, span), jnp.bfloat16),
            pltpu.VMEM((blocks, rows, span), jnp.bfloat16),
            pltpu.VMEM((blocks, rows, span), jnp.bfloat16),
            pltpu.VMEM((blocks, span, chans), jnp.bfloat16),
            pltpu.SemaphoreType.DMA((5 * blocks,)),
        ],
        out_shape=[jax.ShapeDtypeStruct(s, jnp.float32) for s in shapes],
        compiler_params=WHOLE,
        cost_estimate=pl.CostEstimate(
            flops=4 * rows * span * blocks * (chans + 8),
            bytes_accessed=12 * rows * span * blocks,
            transcendentals=0,
        ),
    )(ids, keep, got, own, other, gate, scale, head, *old)


def terms_kernel(split, odd_ref, scale_ref, shift_ref, head_ref, out_ref):
    sums = [0.0, 0.0]
    offset = 0.0
    exact = functools.partial(
        jnp.dot, precision=lax.Precision.HIGHEST, preferred_element_type=jnp.float32
    )
    for b in range(head_ref.shape[0]):
        head = head_ref[b].astype(jnp.float32)
        both = exact(jnp.concatenate([scale_ref[b], shift_ref[b]] * 4), head)
        half = b // split % 2
        sums[half] = sums[half] + both[0:1]
        offset = offset + both[1:2]
    odd = odd_ref[0] == 1
    out_ref[0:1] = jnp.where(odd, sums[1], sums[0])
    out_ref[1:2] = jnp.where(odd, sums[0], sums[1])
    out_ref[2:3] = offset


def finish_kernel(
    model, ids, step_ref, shares_ref, ramps_ref, mine_ref, beside_ref, ahead_ref, got_ref,
    behind_ref, terms_ref, latents_ref, tail_ref, start_ref, out_ref, speed, outer
):
    rows, chans = speed.shape
    frames = latents_ref.shape[0]
    per_frame = rows // frames
    own_cw, their_cw, offset = (terms_ref[i : i + 1] for i in range(3))

    def combine(a, b):
        mid_a, one_a, two_a = (a[:, chans + i : chans + i + 1] for i in range(3))
        mid_b, one_b, two_b = (b[:, chans + i : chans + i + 1] for i in range(3))
        centre = (one_a + one_b) / model + 0.5 * (mid_a + mid_b)
        da = centre - mid_a
        db = centre - mid_b
        half = model // 2
        square = (two_a - 2.0 * da * one_a + half * da * da) + (
            two_b - 2.0 * db * one_b + half * db * db
        )
        inverse = 1.0 / jnp.sqrt(square / model + EPSILON)
        dots = a[:, :chans] + b[:, :chans] - da * own_cw - db * their_cw
        return dots * inverse + offset

    speed[...] = combine(mine_ref[0], got_ref[:rows])
    beside = combine(beside_ref[...], got_ref[rows:])
    outside = combine(ahead_ref[...], behind_ref[...])
    odd = ids[0] == 1
    outer[0] = jnp.where(odd, beside, outside)
    outer[1] = jnp.where(odd, outside, beside)
    step = step_ref[0]
    window = ids[1]
    previous = ids[2]
    over_prev = shares_ref[previous]
    over_next = shares_ref[window]
    frame = lax.broadcasted_iota(jnp.int32, (frames, 1), 0)
    column = lambda scalar: jnp.full((frames, 1), scalar, jnp.int32).astype(jnp.float32)
    zero = jnp.zeros((frames, 1), jnp.float32)
    takes = []
    mine = zero
    theirs = zero
    for j in range(FD):
        at = j - FD + over_prev
        pick = (frame == at) & (frame < over_prev)
        near = jnp.maximum(at, 0)
        takes.append((0, j, pick))
        theirs = jnp.where(pick, column(ramps_ref[previous, 2 * near]), theirs)
        mine = jnp.where(pick, column(ramps_ref[previous, 2 * near + 1]), mine)
    for j in range(FD):
        pick = (frame == j + frames - over_next) & (frame >= over_prev)
        takes.append((1, j, pick))
        mine = jnp.where(pick, column(ramps_ref[window, 2 * j]), mine)
        theirs = jnp.where(pick, column(ramps_ref[window, 2 * j + 1]), theirs)
    alone = mine + theirs == 0.0
    mine = jnp.where(alone, 1.0, mine)
    total = mine + theirs
    for p in range(per_frame):
        lanes = slice(p * chans, (p + 1) * chans)
        fresh = latents_ref[:, lanes] + step * speed[pl.ds(p, frames, stride=per_frame), :]
        sides = [
            ref[:, lanes] + step * outer[side, pl.ds(p, FD, stride=per_frame), :]
            for side, ref in enumerate((tail_ref, start_ref))
        ]
        other = jnp.zeros_like(fresh)
        for side, j, pick in takes:
            other = jnp.where(pick, sides[side][j : j + 1], other)
        out_ref[:, lanes] = (mine * fresh + theirs * other) / total


def after(*values):
    return lax.optimization_barrier(values)


def local(
    queries,
    keys,
    values,
    stream,
    out_weight,
    gate,
    head_shift,
    head_scale,
    head_weight,
    latents,
    step_size,
    intersections,
    ramps,
):
    rows, feat = queries.shape
    groups = lax.axis_size("fsdp")
    count = lax.axis_size("win")
    line = count // 2
    width = out_weight.shape[1]
    model = stream.shape[1]
    chans = head_weight.shape[1]
    cols = feat // groups
    heads = cols // HD
    window = lax.axis_index("win")
    member = lax.axis_index("fsdp")
    z = window // 2
    parity = window % 2
    regroup = width % LANES != 0 or line != 4
    blocks = line
    if regroup:
        blocks = max(b for b in (1, 2, 4) if (model // 2) % (b * LANES) == 0)
    span = model // 2 // blocks

    def group(value, bits):
        return lax.dynamic_slice(value, (0, (member ^ bits) * cols), (rows, cols))

    def pack(bits, *arrays):
        return jnp.stack([group(v, bits) for v in arrays])

    ids = jnp.stack([member, member ^ 2]).astype(jnp.int32)
    if regroup:
        sets = [[2 * a + p for a in range(line)] for p in range(2)]
        full = lax.all_gather(out_weight, "win", axis=1, tiled=True, axis_index_groups=sets)
        near = [[full[:, r * span : (r + 1) * span]] for r in range(blocks)]
        far = [[swap(b[0], "fsdp", 2)] for b in near]
        picks = [0] * blocks
        half_first = lambda v: jnp.swapaxes(v.reshape((line, 2, width) + v.shape[1:]), 0, 1)
        places = [(parity * blocks + r, r) for r in range(blocks)]
        ordered = half_first(stream.T).reshape(model, rows).T
        sent = [(1 - parity) * blocks + r for r in range(blocks)]
    else:
        down = [(a + 1, a) for a in range(line - 1)]
        up = [(a, a + 1) for a in range(line - 1)]
        on_down = [(a - 1, a - 2) for a in range(2, line)]
        on_up = [(a + 1, a + 2) for a in range(line - 2)]
        far_w = swap(out_weight, "fsdp", 2)
        near_up = line_move(out_weight, up)
        near_down = line_move(out_weight, down)
        half_first = lambda v: v
        ordered = stream
        sent = [2 * r + 1 - parity for r in range(blocks)]
    sizes = [(0, 0, heads), (1, 0, (heads + 1) // 2), (1, (heads + 1) // 2, heads // 2)]

    def packed(chunk):
        part, first, size = chunk
        at = slice(first * HD, (first + size) * HD)
        direct = pack(2 if part == 0 else 0, keys, values)[:, :, at]
        cross = pack(3 if part == 0 else 1, keys, values)[:, :, at]
        return direct, cross

    def sends(pair):
        return swap(pair[0], "fsdp", 2), swap(pair[1], "fsdp", 3)

    gate_b = half_first(gate).reshape(2 * blocks, 1, span)
    scale_b = half_first(head_scale).reshape(2 * blocks, 1, span)
    head_b = half_first(head_weight).reshape(2 * blocks, span, chans)
    shift_b = half_first(head_shift).reshape(2 * blocks, 1, span)
    vmem = pl.BlockSpec(memory_space=pltpu.VMEM)
    smem = pl.BlockSpec(memory_space=pltpu.SMEM)
    terms = pl.pallas_call(
        functools.partial(terms_kernel, blocks if regroup else 1),
        in_specs=[smem] + [vmem] * 3,
        out_specs=vmem,
        out_shape=jax.ShapeDtypeStruct((3, chans), jnp.float32),
        compiler_params=WHOLE,
    cost_estimate=pl.CostEstimate(
        flops=100 * model * chans, bytes_accessed=4 * model * chans, transcendentals=0
    ),
    )(parity.reshape(1).astype(jnp.int32), scale_b, shift_b, head_b)
    pair1, pair2 = packed(sizes[1]), packed(sizes[2])

    kv0 = sends(packed(sizes[0]))
    ring = [(i, (i + 1) % count) for i in range(count)]
    tail_latents = lax.ppermute(latents[latents.shape[0] - FD :], "win", ring)
    start_latents = lax.ppermute(latents[:FD], "win", [(j, i) for i, j in ring])
    mate = jnp.stack([pack(1, queries, keys, values), pack(3, queries, keys, values)])
    mate = swap(mate, "fsdp", 1)
    other_stream = jnp.stack(
        [lax.dynamic_slice(ordered, (0, b * span), (rows, span)) for b in sent]
    )
    other_stream = swap(other_stream, "win", 1)
    if not regroup:
        up2 = line_move(near_up, on_up)
        down2 = line_move(near_down, on_down)
        near2 = jnp.where(z >= 2, up2, down2)
        edge = line_move(near2, [(2, 3), (1, 0)])
        far_up = line_move(far_w, up)
        far_down = line_move(far_w, down)
    kv0, pair1 = after(kv0, pair1)
    kv1 = sends(pair1)

    def run(chunk, kv):
        return attend(ids, queries, keys, values, mate, *kv, *chunk, heads)

    att0 = run(sizes[0], kv0)
    att0_x = swap(att0, "win", 1)
    kv2 = sends(pair2)
    att1 = run(sizes[1], kv1)
    att1_x = swap(att1, "win", 1)
    if not regroup:
        ends = [
            ((w * groups + f), (w * groups + (f ^ 2)))
            for w in range(count)
            if w // 2 in (0, line - 1)
            for f in range(groups)
        ]
        far_edge = lax.ppermute(edge, ("win", "fsdp"), ends)
        far_up2 = line_move(far_up, on_up)
        far_down2 = line_move(far_down, on_down)
        at_top = (z == line - 1).astype(jnp.int32)
        at_end = ((z == line - 1) | (z == 0)).astype(jnp.int32)
        upper = (z >= 2).astype(jnp.int32)
        near = [[out_weight], [near_down, near_up], [near2], [near_up, edge]]
        far = [[far_w], [far_down, far_up], [far_down2, far_up2], [far_up, far_edge]]
        picks = [(0, 0), (at_top, at_top), (0, upper), (at_end, at_end)]
        steps = [0, jnp.where(z == line - 1, 3, 1), 2, jnp.where(z == line - 1, 1, 3)]
        places = [(2 * ((z + r) % line) + parity, (z + r) % line) for r in steps]
    else:
        picks = [(0, 0)] * blocks
    att2 = run(sizes[2], kv2)
    att2_x = swap(att2, "win", 1)

    frames = latents.shape[0]
    edge_rows = FD * rows // frames
    table = lambda entries: jnp.stack([jnp.asarray(e, jnp.int32) for e in entries])
    near_ids = table([p[0] for p in picks])
    far_ids = table([p[1] for p in picks])
    spots = table([p[0] for p in places] + [p[1] for p in places] + [parity])
    part = project(near_ids, (0, 1), (att0, att0_x), [[o] for o in near])
    rest = (att1, att2, att1_x, att2_x)
    far = [[o] for o in far]
    given = project(far_ids, (1,), rest, far, part)
    got = swap(given, "fsdp", 1)
    keep = project(far_ids, (0,), rest, far, part)
    sums = tally(spots, keep, got, ordered, other_stream, gate_b, scale_b, head_b, None, edge_rows)
    state = sums[0]
    _, across, ahead, behind, beside = sums
    got = swap(across, "win", 1)
    ahead = lax.ppermute(
        ahead,
        "win",
        [(2 * a + p, 2 * ((a + 1 - 2 * p) % line) + p) for a in range(line) for p in range(2)],
    )
    behind = lax.ppermute(
        behind,
        "win",
        [(2 * a + p, 2 * ((a - 1 + 2 * p) % line) + 1 - p) for a in range(line) for p in range(2)],
    )
    marks = jnp.stack([parity, window, (window + count - 1) % count]).astype(jnp.int32)
    return pl.pallas_call(
        functools.partial(finish_kernel, model),
        in_specs=[smem] * 4 + [vmem] * 9,
        out_specs=vmem,
        scratch_shapes=[
            pltpu.VMEM((rows, chans), jnp.float32),
            pltpu.VMEM((2, edge_rows, chans), jnp.float32),
        ],
        out_shape=jax.ShapeDtypeStruct(latents.shape, jnp.float32),
        compiler_params=WHOLE,
    )(
        marks, step_size, intersections, ramps.reshape(count, -1), state, beside, ahead,
        got, behind, terms, latents, tail_latents, start_latents
    )


def solution(mesh):
    in_specs = (
        P(("win", "fsdp"), None),
        P(("win", "fsdp"), None),
        P(("win", "fsdp"), None),
        P(("win", "fsdp"), None),
        P("fsdp", "win"),
        P(),
        P(),
        P(),
        P(),
        P("win", "fsdp"),
        P(),
        P(),
        P(),
    )
    out_specs = P("win", "fsdp")

    return jax.shard_map(local, mesh=mesh, in_specs=in_specs, out_specs=out_specs, check_vma=False)
```

```python
import functools
import math

import jax
import jax.numpy as jnp
from jax import lax
from jax.experimental import pallas as pl
from jax.experimental.pallas import tpu as pltpu
from jax.sharding import PartitionSpec as P


HD = 128
FD = 4
EPSILON = 0.001
LANES = 128


NEAR = 5
WHOLE = pltpu.CompilerParams(vmem_limit_bytes=67043328)


def swap(value, axis, bits):
    size = lax.axis_size(axis)
    return lax.ppermute(value, axis, [(i, i ^ bits) for i in range(size)])


def line_move(value, moves):
    pairs = [(2 * a + p, 2 * b + p) for a, b in moves for p in range(2)]
    return lax.ppermute(value, "win", pairs)


def attend_kernel(score_scale, q_ref, k_ref, v_ref, mate_ref, far_ref, diag_ref, out_ref):
    factor = score_scale * math.log2(math.e)
    tasks = [(h, half) for h in range(out_ref.shape[2] // HD) for half in range(2)]

    def scores_of(task):
        head, half = task
        cols = slice(head * HD, (head + 1) * HD)
        query = mate_ref[0, 0, :, cols] if half else q_ref[:, cols]
        keys = (k_ref[:, cols], mate_ref[0, 1, :, cols], far_ref[0, :, cols], diag_ref[0, :, cols])
        return [
            lax.dot_general(query, k, (((1,), (1,)), ((), ())), preferred_element_type=jnp.float32)
            for k in keys
        ]

    coming = scores_of(tasks[0])
    for i, (head, half) in enumerate(tasks):
        scores = coming
        if i + 1 < len(tasks):
            coming = scores_of(tasks[i + 1])
        cols = slice(head * HD, (head + 1) * HD)
        values = (
            v_ref[:, cols], mate_ref[0, 2, :, cols], far_ref[1, :, cols], diag_ref[1, :, cols]
        )
        peaks = [jnp.max(s, axis=-1, keepdims=True) for s in scores]
        highest = functools.reduce(jnp.maximum, peaks)
        total = None
        summed = None
        for s, v in zip(scores, values):
            exponent = jnp.exp2((s - highest) * factor)
            part = jnp.sum(exponent, axis=-1, keepdims=True)
            prod = jnp.dot(exponent.astype(jnp.bfloat16), v, preferred_element_type=jnp.float32)
            total = part if total is None else total + part
            summed = prod if summed is None else summed + prod
        out_ref[half, :, cols] = (summed / total).astype(jnp.bfloat16)


def fetching_attend_kernel(
    score_scale, part, first, heads, ids, queries, keys, values, mate, far, diag, out_ref,
    q_ref, k_ref, v_ref, mate_ref, far_ref, diag_ref, sems
):
    width = q_ref.shape[1]
    fetch = Fetch(sems)
    own = pl.ds(pl.multiple_of((ids[part] * heads + first) * HD, HD), width)
    copies = [
        fetch.start(source.at[:, own], place)
        for source, place in ((queries, q_ref), (keys, k_ref), (values, v_ref))
    ]
    group = mate.at[pl.ds(part, 1), :, :, pl.ds(first * HD, width)]
    copies.append(fetch.start(group, mate_ref))
    copies.append(fetch.start(far, far_ref))
    copies.append(fetch.start(diag, diag_ref))
    for copy in copies:
        copy.wait()
    attend_kernel(score_scale, q_ref, k_ref, v_ref, mate_ref, far_ref, diag_ref, out_ref)


def attend(ids, queries, keys, values, mate, far, diag, part, first, count, heads):
    rows = queries.shape[0]
    width = count * HD
    hbm = pl.BlockSpec(memory_space=pltpu.HBM)
    return pl.pallas_call(
        functools.partial(fetching_attend_kernel, 1.0 / math.sqrt(HD), part, first, heads),
        in_specs=[pl.BlockSpec(memory_space=pltpu.SMEM)] + [hbm] * 6,
        out_specs=pl.BlockSpec(memory_space=pltpu.VMEM),
        scratch_shapes=[pltpu.VMEM((rows, width), jnp.bfloat16)] * 3
        + [pltpu.VMEM((1, 3, rows, width), jnp.bfloat16)]
        + [pltpu.VMEM((2, rows, width), jnp.bfloat16)] * 2
        + [pltpu.SemaphoreType.DMA((6,))],
        out_shape=jax.ShapeDtypeStruct((2, rows, width), jnp.bfloat16),
        compiler_params=WHOLE,
        cost_estimate=pl.CostEstimate(
            flops=32 * rows * rows * HD * count,
            bytes_accessed=24 * rows * HD * count,
            transcendentals=8 * rows * rows * count,
        ),
    )(ids, queries, keys, values, mate, far, diag)


class Fetch:
    def __init__(self, sems):
        self.sems = sems
        self.count = 0

    def start(self, source, target):
        copy = pltpu.make_async_copy(source, target, self.sems.at[self.count])
        self.count += 1
        copy.start()
        return copy

    def start_one_of(self, index, sources, target):
        copies = [pltpu.make_async_copy(v, target, self.sems.at[self.count]) for v in sources]
        self.count += 1
        for c, copy in enumerate(copies):
            if len(copies) == 1:
                copy.start()
            else:
                pl.when(index == c)(copy.start)
        return copies[0]


def project_kernel(blocks, chunks, added, ids, *refs):
    att = refs[: 2 * chunks]
    keep_ref, give_ref, side, held, made, before, sems, out_sems = refs[-8:]
    parts = refs[2 * chunks : 2 * chunks + added]
    sources = list(refs[2 * chunks + added : -8])
    _, _, rows, width = side.shape
    depth = width // len(blocks[0])
    fetch = Fetch(sems)
    waits = [[] for _ in blocks]
    for w in range(2):
        start = 0
        for part in att[w * chunks : (w + 1) * chunks]:
            cols = part.shape[-1]
            waits[0].append(fetch.start(part, side.at[:, w, :, pl.ds(start, cols)]))
            start += cols

    def weights(b):
        for j, (entry, count) in enumerate(blocks[b]):
            options = [sources.pop(0) for _ in range(count)]
            place = held.at[b, pl.ds(j * depth, depth), :]
            waits[b].append(fetch.start_one_of(ids[entry], options, place))
        for h, part in enumerate(parts):
            waits[b].append(fetch.start(part.at[b], before.at[b, h]))

    weights(0)
    leaving = []
    for b in range(len(blocks)):
        for copy in waits[b]:
            copy.wait()
        if b + 1 < len(blocks):
            weights(b + 1)
        for h, out_ref in ((1, give_ref), (0, keep_ref)):
            part = jnp.dot(
                side[h].reshape(2 * rows, width), held[b], preferred_element_type=jnp.float32
            )
            for w in range(2):
                piece = part[w * rows : (w + 1) * rows]
                if added:
                    piece = piece + before[b, h, w].astype(jnp.float32)
                made[b, h, w] = piece.astype(jnp.bfloat16)
            copy = pltpu.make_async_copy(made.at[b, h], out_ref.at[b], out_sems.at[b, h])
            copy.start()
            leaving.append(copy)
    for copy in leaving:
        copy.wait()


def project(ids, att, sources, parts=()):
    blocks = tuple(tuple((entry, len(options)) for entry, options in s) for s in sources)
    flat = [v for slots in sources for _, options in slots for v in options]
    depth, span = flat[0].shape
    rows = att[0].shape[1]
    count = len(blocks)
    width = depth * len(blocks[0])
    shape = (count, 2, rows, span)
    hbm = pl.BlockSpec(memory_space=pltpu.HBM)
    return pl.pallas_call(
        functools.partial(project_kernel, blocks, len(att) // 2, len(parts)),
        in_specs=[pl.BlockSpec(memory_space=pltpu.SMEM)]
        + [hbm] * (len(att) + len(parts) + len(flat)),
        out_specs=[hbm] * 2,
        scratch_shapes=[
            pltpu.VMEM((2, 2, rows, width), jnp.bfloat16),
            pltpu.VMEM((count, width, span), jnp.bfloat16),
            pltpu.VMEM(shape[:1] + (2,) + shape[1:], jnp.bfloat16),
            pltpu.VMEM((count if parts else 1, 2) + shape[1:], jnp.bfloat16),
            pltpu.SemaphoreType.DMA((len(att) + count * (len(blocks[0]) + len(parts)),)),
            pltpu.SemaphoreType.DMA((count, 2)),
        ],
        out_shape=[jax.ShapeDtypeStruct(shape, jnp.bfloat16)] * 2,
        compiler_params=WHOLE,
        cost_estimate=pl.CostEstimate(
            flops=8 * rows * width * span * count,
            bytes_accessed=8 * rows * width + 2 * count * width * span,
            transcendentals=0,
        ),
    )(ids, *att, *parts, *flat)


def tally_kernel(first, last, arrays, spots, ids, *refs):
    keeps, gots, refs = refs[:arrays], refs[arrays : 2 * arrays], refs[2 * arrays :]
    own_ref, other_ref, gate_ref, scale_ref, head_ref = refs[:5]
    state_ref = None if first else refs[5]
    out_refs = refs[5 + (not first) : -6]
    keep, got, own, other, head, sems = refs[-6:]
    _, _, rows, span = keep.shape
    chans = head_ref.shape[2]
    fetch = Fetch(sems)
    place = [ids[spot[2]] for spot in spots]
    waits = []
    for b, (array, at, _, row) in enumerate(spots):
        column = pl.ds(pl.multiple_of(place[b] * span, LANES), span)
        waits.append(
            [
                fetch.start(keeps[array].at[at], keep.at[b]),
                fetch.start(gots[array].at[at], got.at[b]),
                fetch.start(own_ref.at[:, column], own.at[b]),
                fetch.start(other_ref.at[ids[row]], other.at[b]),
                fetch.start(head_ref.at[place[b]], head.at[b]),
            ]
        )
    state = [None] * 2
    if not first:
        for w in range(2):
            old = state_ref[w]
            parts = [old[:, chans + i : chans + i + 1] for i in range(3)]
            state[w] = tuple(parts) + (old[:, :chans],)
    for b in range(len(spots)):
        for copy in waits[b]:
            copy.wait()
        gate = gate_ref[place[b]]
        scale = scale_ref[place[b]]
        for w, stream in enumerate((own, other)):
            proj = keep[b, w].astype(jnp.float32) + got[b, w].astype(jnp.float32)
            hidden = stream[b].astype(jnp.float32) + gate * proj
            if state[w] is None:
                centre = jnp.mean(hidden, axis=-1, keepdims=True)
            else:
                centre = state[w][0]
            moved = hidden - centre
            dots = jnp.dot(
                (moved * scale).astype(jnp.bfloat16), head[b], preferred_element_type=jnp.float32
            )
            one = jnp.sum(moved, axis=-1, keepdims=True)
            two = jnp.sum(moved * moved, axis=-1, keepdims=True)
            if state[w] is not None:
                one, two, dots = one + state[w][1], two + state[w][2], dots + state[w][3]
            state[w] = (centre, one, two, dots)
    sums_ref = out_refs[0]
    for w, (centre, one, two, dots) in enumerate(state):
        sums_ref[w, :, :chans] = dots
        lane = lax.broadcasted_iota(jnp.int32, (rows, sums_ref.shape[2] - chans), 1)
        sums_ref[w, :, chans:] = jnp.where(
            lane == 0, centre, jnp.where(lane == 1, one, jnp.where(lane == 2, two, 0.0))
        )
    if last is not None:
        across_ref, ahead_ref, behind_ref, beside_ref = out_refs[1:]
        edge = ahead_ref.shape[0]
        odd = ids[last]
        inner = pl.ds(pl.multiple_of((1 - odd) * (rows - edge), 8), edge)
        outer = pl.ds(pl.multiple_of(odd * (rows - edge), 8), edge)
        across_ref[:rows] = sums_ref[1]
        across_ref[rows:] = sums_ref[0, inner]
        ahead_ref[...] = sums_ref[1, inner]
        behind_ref[...] = sums_ref[0, outer]
        beside_ref[...] = sums_ref[1, outer]


def tally(ids, spots, keeps, gots, own, other, gate, scale, head, state, last, edge):
    _, _, rows, span = keeps[0].shape
    count = len(spots)
    chans = head.shape[2]
    lanes = chans + LANES - chans % LANES
    old = [] if state is None else [state]
    hbm = pl.BlockSpec(memory_space=pltpu.HBM)
    near_by = pl.BlockSpec(memory_space=pltpu.VMEM)
    shapes = [(2, rows, lanes)]
    if last is not None:
        shapes += [(rows + edge, lanes)] + [(edge, lanes)] * 3
    return pl.pallas_call(
        functools.partial(tally_kernel, state is None, last, len(keeps), spots),
        in_specs=[pl.BlockSpec(memory_space=pltpu.SMEM)]
        + [hbm] * (2 * len(keeps) + 2)
        + [near_by] * 2
        + [hbm]
        + [near_by] * len(old),
        out_specs=[near_by] * len(shapes),
        scratch_shapes=[
            pltpu.VMEM((count, 2, rows, span), jnp.bfloat16),
            pltpu.VMEM((count, 2, rows, span), jnp.bfloat16),
            pltpu.VMEM((count, rows, span), jnp.bfloat16),
            pltpu.VMEM((count, rows, span), jnp.bfloat16),
            pltpu.VMEM((count, span, chans), jnp.bfloat16),
            pltpu.SemaphoreType.DMA((5 * count,)),
        ],
        out_shape=[jax.ShapeDtypeStruct(s, jnp.float32) for s in shapes],
        compiler_params=WHOLE,
        cost_estimate=pl.CostEstimate(
            flops=4 * rows * span * count * (chans + 8),
            bytes_accessed=12 * rows * span * count,
            transcendentals=0,
        ),
    )(ids, *keeps, *gots, own, other, gate, scale, head, *old)


def terms_kernel(split, ids, scale_ref, shift_ref, head_ref, out_ref):
    sums = [0.0, 0.0]
    offset = 0.0
    exact = functools.partial(
        jnp.dot, precision=lax.Precision.HIGHEST, preferred_element_type=jnp.float32
    )
    for b in range(head_ref.shape[0]):
        head = head_ref[b].astype(jnp.float32)
        both = exact(jnp.concatenate([scale_ref[b], shift_ref[b]] * 4), head)
        half = b // split % 2
        sums[half] = sums[half] + both[0:1]
        offset = offset + both[1:2]
    odd = ids[2] == 1
    out_ref[0:1] = jnp.where(odd, sums[1], sums[0])
    out_ref[1:2] = jnp.where(odd, sums[0], sums[1])
    out_ref[2:3] = offset


def finish_kernel(
    model, ids, step_ref, shares_ref, ramps_ref, mine_ref, beside_ref, ahead_ref, got_ref,
    behind_ref, terms_ref, latents_ref, tail_ref, start_ref, out_ref, speed, outer
):
    rows, chans = speed.shape
    frames = latents_ref.shape[0]
    per_frame = rows // frames
    own_cw, their_cw, offset = (terms_ref[i : i + 1] for i in range(3))

    def combine(a, b):
        mid_a, one_a, two_a = (a[:, chans + i : chans + i + 1] for i in range(3))
        mid_b, one_b, two_b = (b[:, chans + i : chans + i + 1] for i in range(3))
        centre = (one_a + one_b) / model + 0.5 * (mid_a + mid_b)
        da = centre - mid_a
        db = centre - mid_b
        half = model // 2
        square = (two_a - 2.0 * da * one_a + half * da * da) + (
            two_b - 2.0 * db * one_b + half * db * db
        )
        inverse = 1.0 / jnp.sqrt(square / model + EPSILON)
        dots = a[:, :chans] + b[:, :chans] - da * own_cw - db * their_cw
        return dots * inverse + offset

    speed[...] = combine(mine_ref[0], got_ref[:rows])
    beside = combine(beside_ref[...], got_ref[rows:])
    outside = combine(ahead_ref[...], behind_ref[...])
    odd = ids[2] == 1
    outer[0] = jnp.where(odd, beside, outside)
    outer[1] = jnp.where(odd, outside, beside)
    step = step_ref[0]
    window = ids[3]
    previous = ids[4]
    over_prev = shares_ref[previous]
    over_next = shares_ref[window]
    frame = lax.broadcasted_iota(jnp.int32, (frames, 1), 0)
    column = lambda scalar: jnp.full((frames, 1), scalar, jnp.int32).astype(jnp.float32)
    zero = jnp.zeros((frames, 1), jnp.float32)
    takes = []
    mine = zero
    theirs = zero
    for j in range(FD):
        at = j - FD + over_prev
        pick = (frame == at) & (frame < over_prev)
        near = jnp.maximum(at, 0)
        takes.append((0, j, pick))
        theirs = jnp.where(pick, column(ramps_ref[previous, 2 * near]), theirs)
        mine = jnp.where(pick, column(ramps_ref[previous, 2 * near + 1]), mine)
    for j in range(FD):
        pick = (frame == j + frames - over_next) & (frame >= over_prev)
        takes.append((1, j, pick))
        mine = jnp.where(pick, column(ramps_ref[window, 2 * j]), mine)
        theirs = jnp.where(pick, column(ramps_ref[window, 2 * j + 1]), theirs)
    alone = mine + theirs == 0.0
    mine = jnp.where(alone, 1.0, mine)
    total = mine + theirs
    for p in range(per_frame):
        lanes = slice(p * chans, (p + 1) * chans)
        fresh = latents_ref[:, lanes] + step * speed[pl.ds(p, frames, stride=per_frame), :]
        sides = [
            ref[:, lanes] + step * outer[side, pl.ds(p, FD, stride=per_frame), :]
            for side, ref in enumerate((tail_ref, start_ref))
        ]
        other = jnp.zeros_like(fresh)
        for side, j, pick in takes:
            other = jnp.where(pick, sides[side][j : j + 1], other)
        out_ref[:, lanes] = (mine * fresh + theirs * other) / total


def after(*values):
    return lax.optimization_barrier(values)


def local(
    queries,
    keys,
    values,
    stream,
    out_weight,
    gate,
    head_shift,
    head_scale,
    head_weight,
    latents,
    step_size,
    intersections,
    ramps,
):
    rows, feat = queries.shape
    groups = lax.axis_size("fsdp")
    count = lax.axis_size("win")
    line = count // 2
    width = out_weight.shape[1]
    model = stream.shape[1]
    chans = head_weight.shape[1]
    cols = feat // groups
    heads = cols // HD
    window = lax.axis_index("win")
    member = lax.axis_index("fsdp")
    z = window // 2
    parity = window % 2
    regroup = width % LANES != 0 or line != 4
    blocks = line
    if regroup:
        blocks = max(b for b in (1, 2, 4) if (model // 2) % (b * LANES) == 0)
    span = model // 2 // blocks

    def group(value, bits):
        return lax.dynamic_slice(value, (0, (member ^ bits) * cols), (rows, cols))

    def pack(bits, *arrays):
        return jnp.stack([group(v, bits) for v in arrays])

    if regroup:
        sets = [[2 * a + p for a in range(line)] for p in range(2)]
        full = lax.all_gather(out_weight, "win", axis=1, tiled=True, axis_index_groups=sets)
        near = [[full[:, r * span : (r + 1) * span]] for r in range(blocks)]
        far = [[swap(b[0], "fsdp", 2)] for b in near]
        picks = [0] * blocks
        half_first = lambda v: jnp.swapaxes(v.reshape((line, 2, width) + v.shape[1:]), 0, 1)
        places = [(parity * blocks + r, r) for r in range(blocks)]
        ordered = half_first(stream.T).reshape(model, rows).T
        sent = [(1 - parity) * blocks + r for r in range(blocks)]
    else:
        down = [(a + 1, a) for a in range(line - 1)]
        up = [(a, a + 1) for a in range(line - 1)]
        on_down = [(a - 1, a - 2) for a in range(2, line)]
        on_up = [(a + 1, a + 2) for a in range(line - 2)]
        far_w = swap(out_weight, "fsdp", 2)
        near_up = line_move(out_weight, up)
        near_down = line_move(out_weight, down)
        half_first = lambda v: v
        ordered = stream
        sent = [2 * r + 1 - parity for r in range(blocks)]
    if not regroup:
        at_top = (z == line - 1).astype(jnp.int32)
        at_end = ((z == line - 1) | (z == 0)).astype(jnp.int32)
        picks = [(0, 0), (at_top, at_top), (0, 0), (at_end, at_end)]
        steps = [0, jnp.where(z == line - 1, 3, 1), 2, jnp.where(z == line - 1, 1, 3)]
        places = [(2 * ((z + r) % line) + parity, (z + r) % line) for r in steps]
    else:
        picks = [(0, 0)] * blocks
    ids = [member, member ^ 2, parity, window, (window + count - 1) % count]
    ids += [p[0] for p in picks] + [p[1] for p in picks]
    ids += [p[0] for p in places] + [p[1] for p in places]
    ids = jnp.stack([jnp.asarray(e, jnp.int32) for e in ids])
    sizes = [(0, 0, heads), (1, 0, (heads + 1) // 2), (1, (heads + 1) // 2, heads // 2)]

    def packed(chunk):
        part, first, size = chunk
        at = slice(first * HD, (first + size) * HD)
        direct = pack(2 if part == 0 else 0, keys, values)[:, :, at]
        cross = pack(3 if part == 0 else 1, keys, values)[:, :, at]
        return direct, cross

    def sends(pair):
        return swap(pair[0], "fsdp", 2), swap(pair[1], "fsdp", 3)

    gate_b = half_first(gate).reshape(2 * blocks, 1, span)
    scale_b = half_first(head_scale).reshape(2 * blocks, 1, span)
    head_b = half_first(head_weight).reshape(2 * blocks, span, chans)
    shift_b = half_first(head_shift).reshape(2 * blocks, 1, span)
    vmem = pl.BlockSpec(memory_space=pltpu.VMEM)
    smem = pl.BlockSpec(memory_space=pltpu.SMEM)
    terms = pl.pallas_call(
        functools.partial(terms_kernel, blocks if regroup else 1),
        in_specs=[smem] + [vmem] * 3,
        out_specs=vmem,
        out_shape=jax.ShapeDtypeStruct((3, chans), jnp.float32),
        compiler_params=WHOLE,
    cost_estimate=pl.CostEstimate(
        flops=100 * model * chans, bytes_accessed=4 * model * chans, transcendentals=0
    ),
    )(ids, scale_b, shift_b, head_b)
    pair1, pair2 = packed(sizes[1]), packed(sizes[2])

    kv0 = sends(packed(sizes[0]))
    ring = [(i, (i + 1) % count) for i in range(count)]
    tail_latents = lax.ppermute(latents[latents.shape[0] - FD :], "win", ring)
    start_latents = lax.ppermute(latents[:FD], "win", [(j, i) for i, j in ring])
    mate = jnp.stack([pack(1, queries, keys, values), pack(3, queries, keys, values)])
    mate = swap(mate, "fsdp", 1)
    other_stream = jnp.stack(
        [lax.dynamic_slice(ordered, (0, b * span), (rows, span)) for b in sent]
    )
    other_stream = swap(other_stream, "win", 1)
    if not regroup:
        up2 = line_move(near_up, on_up)
        down2 = line_move(near_down, on_down)
        near2 = jnp.where(z >= 2, up2, down2)
        edge = line_move(near2, [(2, 3), (1, 0)])
        far_up = line_move(far_w, up)
        far_down = line_move(far_w, down)
        far_two = line_move(far_w, [(a, (a + 2) % line) for a in range(line)])
    kv0, pair1, pair2 = after(kv0, pair1, pair2)
    kv1 = sends(pair1)

    def run(chunk, kv):
        return attend(ids, queries, keys, values, mate, *kv, *chunk, heads)

    att0 = run(sizes[0], kv0)
    att0_x = swap(att0, "win", 1)
    kv2 = sends(pair2)
    att1 = run(sizes[1], kv1)
    att1_x = swap(att1, "win", 1)
    if not regroup:
        ends = [
            ((w * groups + f), (w * groups + (f ^ 2)))
            for w in range(count)
            if w // 2 in (0, line - 1)
            for f in range(groups)
        ]
        far_edge = lax.ppermute(edge, ("win", "fsdp"), ends)
        near = [[out_weight], [near_down, near_up], [near2], [near_up, edge]]
        far = [[far_w], [far_down, far_up], [far_two], [far_up, far_edge]]
    att2 = run(sizes[2], kv2)
    att2_x = swap(att2, "win", 1)

    frames = latents.shape[0]
    edge_rows = FD * rows // frames
    split = (blocks + 1) // 2
    plans = [list(range(split)), list(range(split, blocks))]
    plans = [now for now in plans if now]
    tallies = [list(range(blocks))]
    slots = lambda b: [(NEAR + b, near[b]), (NEAR + blocks + b, far[b])]
    made = {}
    if len(plans) > 1:
        parts = project(ids, (att0, att0_x), [slots(b)[:1] for b in plans[1]])
    for i, now in enumerate(plans):
        if i == 0:
            attended = (att0, att1, att2, att0_x, att1_x, att2_x)
            keep, given = project(ids, attended, [slots(b) for b in now])
        else:
            attended = (att1, att2, att1_x, att2_x)
            keep, given = project(ids, attended, [slots(b)[1:] for b in now], parts)
        got = swap(given, "fsdp", 1)
        made.update({b: (i, keep, got, at) for at, b in enumerate(now)})
    state = None
    for i, now in enumerate(tallies):
        arrays = sorted({made[b][0] for b in now})
        spots = tuple(
            (arrays.index(made[b][0]), made[b][3], NEAR + 2 * blocks + b, NEAR + 3 * blocks + b)
            for b in now
        )
        pairs = {made[b][0]: made[b][1:3] for b in now}
        keeps, gots = zip(*(pairs[a] for a in arrays))
        last = 2 if i + 1 == len(tallies) else None
        sums = tally(
            ids, spots, keeps, gots, ordered, other_stream, gate_b, scale_b, head_b, state,
            last, edge_rows,
        )
        state = sums[0]
    _, across, ahead, behind, beside = sums
    got = swap(across, "win", 1)
    ahead = lax.ppermute(
        ahead,
        "win",
        [(2 * a + p, 2 * ((a + 1 - 2 * p) % line) + p) for a in range(line) for p in range(2)],
    )
    behind = lax.ppermute(
        behind,
        "win",
        [(2 * a + p, 2 * ((a - 1 + 2 * p) % line) + 1 - p) for a in range(line) for p in range(2)],
    )
    return pl.pallas_call(
        functools.partial(finish_kernel, model),
        in_specs=[smem] * 4 + [vmem] * 9,
        out_specs=vmem,
        scratch_shapes=[
            pltpu.VMEM((rows, chans), jnp.float32),
            pltpu.VMEM((2, edge_rows, chans), jnp.float32),
        ],
        out_shape=jax.ShapeDtypeStruct(latents.shape, jnp.float32),
        compiler_params=WHOLE,
    )(
        ids, step_size, intersections, ramps.reshape(count, -1), state, beside, ahead,
        got, behind, terms, latents, tail_latents, start_latents
    )


def solution(mesh):
    in_specs = (
        P(("win", "fsdp"), None),
        P(("win", "fsdp"), None),
        P(("win", "fsdp"), None),
        P(("win", "fsdp"), None),
        P("fsdp", "win"),
        P(),
        P(),
        P(),
        P(),
        P("win", "fsdp"),
        P(),
        P(),
        P(),
    )
    out_specs = P("win", "fsdp")

    return jax.shard_map(local, mesh=mesh, in_specs=in_specs, out_specs=out_specs, check_vma=False)
```
